16 devices in a mesh: dp: 4 (over z, y), tp: 4 (over x, core).
Axes of the slice: x: 2, y: 2, z: 2, core: 2. Of those that a mesh axis runs over, the one named last changes fastest.
Arguments:
- x_in: bfloat16 [4, 2048, 6144], P('dp', 'tp'), parts along dimension 0
- start_pos: int32 [4], P('dp'), parts along dimension 0
- k_cache: bfloat16 [4, 4096, 8, 128], P('dp', None, 'tp'), parts along dimension 0
- v_cache: bfloat16 [4, 4096, 8, 128], P('dp', None, 'tp'), parts along dimension 0
- attn_gain: bfloat16 [6144], replicated
- w_query: bfloat16 [6144, 48, 128], P(None, 'tp')
- w_key: bfloat16 [6144, 8, 128], P(None, 'tp')
- w_value: bfloat16 [6144, 8, 128], P(None, 'tp')
- w_out: bfloat16 [48, 128, 6144], P('tp')
- mlp_gain: bfloat16 [6144], replicated
- w_gate: bfloat16 [6144, 16384], P(None, 'tp')
- w_up: bfloat16 [6144, 16384], P(None, 'tp')
- w_down: bfloat16 [16384, 6144], P('tp')
Outputs:
- output 1: bfloat16 [4, 2048, 6144], P('dp', 'tp'), parts along dimension 0
- output 2: bfloat16 [4, 4096, 8, 128], P('dp', None, 'tp'), parts along dimension 0
- output 3: bfloat16 [4, 4096, 8, 128], P('dp', None, 'tp'), parts along dimension 0
There are 4 independent parts. The reference program is written for one: setup_inputs(seed, part) draws one part's arguments, and reference() takes and returns one part's arrays. A program takes and returns all parts, laid end to end along the dimension named above; an argument that names none is the same for every part.
All inputs are finite; a program needn't handle non-finite values.
Results may differ from the reference program's by a relative error of at most 0.013112.
Values are sent between devices in bfloat16 or wider.
A program may use at most 1 GiB of HBM per device.

```python
import jax
import jax.numpy as jnp
from jax import lax

MODEL_DIM = 6144
Q_HEADS = 48
KV_HEADS = 8
HEAD_DIM = 128
FFN_DIM = 16384
WINDOW = 4096
BATCH_ROWS = 1
CHUNK_LEN = 2048
ROPE_BASE = 10000.0
NORM_EPS = 1e-5
GROUP_SIZE = Q_HEADS // KV_HEADS
QUERY_BLOCK = min(CHUNK_LEN, 128)


def setup_inputs(seed: int = 0, part: int = 0) -> dict:
    part_keys = jax.random.split(jax.random.fold_in(jax.random.key(seed), part), 6)
    shared_keys = jax.random.split(jax.random.key(seed + 1), 9)
    cache_shape = (BATCH_ROWS, WINDOW, KV_HEADS, HEAD_DIM)
    x_in = jax.random.normal(part_keys[0], (BATCH_ROWS, CHUNK_LEN, MODEL_DIM), jnp.float32)
    row_starts = jax.random.randint(part_keys[1], (BATCH_ROWS,), 0, 3 * WINDOW)
    first_start = jax.random.randint(part_keys[2], (), WINDOW, 3 * WINDOW)
    start_pos = jnp.where(jnp.arange(BATCH_ROWS) == 0, first_start, row_starts)
    k_cache = 1.5 * jax.random.normal(part_keys[3], cache_shape, jnp.float32)
    v_mean = jax.random.normal(part_keys[4], (BATCH_ROWS, 1, KV_HEADS, HEAD_DIM), jnp.float32)
    v_cache = v_mean + jax.random.normal(part_keys[5], cache_shape, jnp.float32)
    attn_gain = 1.0 + 0.25 * jax.random.normal(shared_keys[0], (MODEL_DIM,), jnp.float32)
    w_query = (1.5 * MODEL_DIM ** -0.5) * jax.random.normal(shared_keys[1], (MODEL_DIM, Q_HEADS, HEAD_DIM), jnp.float32)
    w_key = (1.5 * MODEL_DIM ** -0.5) * jax.random.normal(shared_keys[2], (MODEL_DIM, KV_HEADS, HEAD_DIM), jnp.float32)
    w_value = MODEL_DIM ** -0.5 * jax.random.normal(shared_keys[3], (MODEL_DIM, KV_HEADS, HEAD_DIM), jnp.float32)
    w_out = (Q_HEADS * HEAD_DIM) ** -0.5 * jax.random.normal(shared_keys[4], (Q_HEADS, HEAD_DIM, MODEL_DIM), jnp.float32)
    mlp_gain = 1.0 + 0.25 * jax.random.normal(shared_keys[5], (MODEL_DIM,), jnp.float32)
    w_gate = MODEL_DIM ** -0.5 * jax.random.normal(shared_keys[6], (MODEL_DIM, FFN_DIM), jnp.float32)
    w_up = MODEL_DIM ** -0.5 * jax.random.normal(shared_keys[7], (MODEL_DIM, FFN_DIM), jnp.float32)
    w_down = FFN_DIM ** -0.5 * jax.random.normal(shared_keys[8], (FFN_DIM, MODEL_DIM), jnp.float32)
    return {
        'x_in': x_in.astype(jnp.bfloat16),
        'start_pos': start_pos.astype(jnp.int32),
        'k_cache': k_cache.astype(jnp.bfloat16),
        'v_cache': v_cache.astype(jnp.bfloat16),
        'attn_gain': attn_gain.astype(jnp.bfloat16),
        'w_query': w_query.astype(jnp.bfloat16),
        'w_key': w_key.astype(jnp.bfloat16),
        'w_value': w_value.astype(jnp.bfloat16),
        'w_out': w_out.astype(jnp.bfloat16),
        'mlp_gain': mlp_gain.astype(jnp.bfloat16),
        'w_gate': w_gate.astype(jnp.bfloat16),
        'w_up': w_up.astype(jnp.bfloat16),
        'w_down': w_down.astype(jnp.bfloat16),
    }


def rms_norm(rows, gain):
    rows32 = rows.astype(jnp.float32)
    inv_rms = lax.rsqrt(jnp.mean(rows32 * rows32, axis=-1, keepdims=True) + NORM_EPS)
    return (rows32 * inv_rms * gain.astype(jnp.float32)).astype(jnp.bfloat16)


def rotate(heads_in, positions):
    inv_freq = jnp.power(ROPE_BASE, -jnp.arange(0, HEAD_DIM, 2).astype(jnp.float32) / HEAD_DIM)
    angles = positions.astype(jnp.float32)[:, None] * inv_freq[None, :]
    cos_t = jnp.cos(angles)[:, None, :]
    sin_t = jnp.sin(angles)[:, None, :]
    pairs = heads_in.reshape(heads_in.shape[0], heads_in.shape[1], HEAD_DIM // 2, 2)
    even = pairs[..., 0]
    odd = pairs[..., 1]
    turned = jnp.stack([even * cos_t - odd * sin_t, even * sin_t + odd * cos_t], axis=-1)
    return turned.reshape(heads_in.shape)


def layer_row(x_row, start, k_old, v_old, attn_gain, w_query, w_key, w_value, w_out, mlp_gain, w_gate, w_up, w_down):
    positions = start + jnp.arange(CHUNK_LEN)
    normed = rms_norm(x_row, attn_gain)
    q_lin = jnp.dot(normed, w_query.reshape(MODEL_DIM, Q_HEADS * HEAD_DIM), preferred_element_type=jnp.float32)
    k_lin = jnp.dot(normed, w_key.reshape(MODEL_DIM, KV_HEADS * HEAD_DIM), preferred_element_type=jnp.float32)
    v_lin = jnp.dot(normed, w_value.reshape(MODEL_DIM, KV_HEADS * HEAD_DIM), preferred_element_type=jnp.float32)
    queries = rotate(q_lin.reshape(CHUNK_LEN, Q_HEADS, HEAD_DIM), positions).astype(jnp.bfloat16)
    k_chunk = rotate(k_lin.reshape(CHUNK_LEN, KV_HEADS, HEAD_DIM), positions).astype(jnp.bfloat16)
    v_chunk = v_lin.astype(jnp.bfloat16).reshape(CHUNK_LEN, KV_HEADS, HEAD_DIM)
    offsets = jnp.mod(jnp.arange(WINDOW) - start, WINDOW)
    cache_valid = (start - WINDOW + offsets) >= 0
    keys = jnp.concatenate([k_old, k_chunk], axis=0).astype(jnp.float32)
    values = jnp.concatenate([v_old, v_chunk], axis=0).astype(jnp.float32)
    n_blocks = CHUNK_LEN // QUERY_BLOCK
    q_tiles = queries.reshape(n_blocks, QUERY_BLOCK, KV_HEADS, GROUP_SIZE, HEAD_DIM)

    def attend_block(tile_pair):
        q_tile, block = tile_pair
        q_ids = block * QUERY_BLOCK + jnp.arange(QUERY_BLOCK)
        cache_mask = cache_valid[None, :] & (offsets[None, :] > q_ids[:, None])
        chunk_mask = jnp.arange(CHUNK_LEN)[None, :] <= q_ids[:, None]
        mask = jnp.concatenate([cache_mask, chunk_mask], axis=1)
        scores = jnp.einsum('qkge,ske->kgqs', q_tile.astype(jnp.float32), keys) * (HEAD_DIM ** -0.5)
        scores = jnp.where(mask[None, None], scores, -jnp.inf)
        attn_probs = jax.nn.softmax(scores, axis=-1).astype(jnp.bfloat16)
        mixed = jnp.einsum('kgqs,ske->qkge', attn_probs.astype(jnp.float32), values)
        return mixed.astype(jnp.bfloat16)

    mixed = lax.map(attend_block, (q_tiles, jnp.arange(n_blocks)))
    attn_out = jnp.dot(mixed.reshape(CHUNK_LEN, Q_HEADS * HEAD_DIM), w_out.reshape(Q_HEADS * HEAD_DIM, MODEL_DIM), preferred_element_type=jnp.float32)
    hidden = (x_row.astype(jnp.float32) + attn_out).astype(jnp.bfloat16)
    mlp_rows = rms_norm(hidden, mlp_gain)
    gate = jnp.dot(mlp_rows, w_gate, preferred_element_type=jnp.float32)
    up_proj = jnp.dot(mlp_rows, w_up, preferred_element_type=jnp.float32)
    activated = (jax.nn.silu(gate) * up_proj).astype(jnp.bfloat16)
    mlp_out = jnp.dot(activated, w_down, preferred_element_type=jnp.float32)
    x_out = (hidden.astype(jnp.float32) + mlp_out).astype(jnp.bfloat16)
    slots = jnp.mod(start + jnp.arange(CHUNK_LEN), WINDOW)
    k_new = k_old.at[slots].set(k_chunk)
    v_new = v_old.at[slots].set(v_chunk)
    return x_out, k_new, v_new


def reference(x_in, start_pos, k_cache, v_cache, attn_gain, w_query, w_key, w_value, w_out, mlp_gain, w_gate, w_up, w_down):
    def one_row(row_inputs):
        x_row, start, k_old, v_old = row_inputs
        return layer_row(x_row, start, k_old, v_old, attn_gain, w_query, w_key, w_value, w_out, mlp_gain, w_gate, w_up, w_down)

    x_out, k_new, v_new = lax.map(one_row, (x_in, start_pos, k_cache, v_cache))
    return x_out, k_new, v_new
```

```python
import functools

import jax
import jax.numpy as jnp
from jax import lax
from jax.experimental import pallas as pl
from jax.experimental.pallas import tpu as pltpu
from jax.sharding import PartitionSpec as P

ROPE_BASE = 10000.0
NORM_EPS = 1e-5
NEG = -1e30


def attn_kernel(start_ref, q_ref, cos_ref, sin_ref, k_ref, v_ref, o_ref, q_s, m_s, l_s, acc_s, *,
                seg_len, first, tile, group, window, plan, halves, cexp):
    d = pl.program_id(1)
    i0 = pl.multiple_of(d * seg_len + first, tile)
    hd = k_ref.shape[-1]
    rows = tile * group
    hrows = rows // halves
    lane = lax.broadcasted_iota(jnp.int32, (tile, hd), 1)
    even = lax.rem(lane, 2) == 0
    cos = cos_ref[...]
    sin = sin_ref[...]
    for g in range(group):
        qh = q_ref[:, g * hd:(g + 1) * hd]
        sw = jnp.where(even, pltpu.roll(qh, hd - 1, 1), pltpu.roll(qh, 1, 1))
        q_s[g * tile:(g + 1) * tile, :] = (qh * cos + sw * sin).astype(jnp.bfloat16)
    m_s[...] = jnp.full_like(m_s, NEG)
    l_s[...] = jnp.zeros_like(l_s)
    acc_s[...] = jnp.zeros_like(acc_s)
    r = lax.broadcasted_iota(jnp.int32, (tile, tile), 0)
    c = lax.broadcasted_iota(jnp.int32, (tile, tile), 1)

    def block(off, width, lo, hi, floor):
        kb = k_ref[0, pl.ds(i0 + off, width), :]
        vb = v_ref[0, pl.ds(i0 + off, width), :]
        for p in range(halves):
            sl = pl.ds(p * hrows, hrows)
            s = lax.dot_general(q_s[sl, :], kb, (((1,), (1,)), ((), ())), preferred_element_type=jnp.float32)
            reps = hrows // tile
            if lo or hi or floor is not None:
                s3 = s.reshape(reps, tile, width)
                if lo:
                    piece = jnp.where((c > r)[None], s3[:, :, :tile], NEG)
                    s3 = jnp.concatenate([piece, s3[:, :, tile:]], axis=2) if width > tile else piece
                if hi:
                    piece = jnp.where((c <= r)[None], s3[:, :, width - tile:], NEG)
                    s3 = jnp.concatenate([s3[:, :, :width - tile], piece], axis=2) if width > tile else piece
                if floor is not None:
                    vid = i0 + off + lax.broadcasted_iota(jnp.int32, (1, 1, width), 2)
                    s3 = jnp.where(vid >= floor, s3, NEG)
                s = s3.reshape(hrows, width)
            m_prev = m_s[sl, :]
            m_new = jnp.maximum(m_prev, jnp.max(s, axis=1, keepdims=True))
            m_s[sl, :] = m_new
            alpha = jnp.exp2((m_prev - m_new) * cexp)
            pr = jnp.exp2((s - jnp.tile(m_new, (1, width // hd))) * cexp)
            part = pr[:, :hd]
            for t in range(1, width // hd):
                part = part + pr[:, t * hd:(t + 1) * hd]
            l_s[sl, :] = l_s[sl, :] * alpha + part
            pv = lax.dot_general(pr.astype(jnp.bfloat16), vb, (((1,), (0,)), ((), ())), preferred_element_type=jnp.float32)
            acc_s[sl, :] = acc_s[sl, :] * alpha + pv

    head, mid, n_mid, tail = plan

    def sweep(floor):
        block(head + mid * n_mid, tail, False, True, floor)
        def body(t, carry):
            block(pl.multiple_of(head + t * mid, tile), mid, False, False, floor)
            return carry
        lax.fori_loop(0, n_mid, body, 0)
        block(0, head, True, False, floor)

    lowest = window - start_ref[0]

    @pl.when(lowest <= i0)
    def _():
        sweep(None)

    @pl.when(lowest > i0)
    def _():
        sweep(lowest)

    for g in range(group):
        sl = pl.ds(g * tile, tile)
        total = jnp.sum(l_s[sl, :], axis=1, keepdims=True)
        o_ref[:, g * hd:(g + 1) * hd] = (acc_s[sl, :] / total).astype(jnp.bfloat16)


def attention(q_lin, cos, sin, k_all, v_all, start, *, segs, seg_len, first, tile, heads, window, plan, halves):
    kv, keys, hd = k_all.shape
    group = heads // kv
    assert plan[0] + plan[1] * plan[2] + plan[3] == window + tile
    kern = functools.partial(attn_kernel, seg_len=seg_len, first=first, tile=tile, group=group, window=window,
                             plan=plan, halves=halves, cexp=float(hd ** -0.5 * 1.4426950408889634))
    rows = tile * group
    step = seg_len // tile
    base = first // tile
    return pl.pallas_call(
        kern,
        out_shape=jax.ShapeDtypeStruct((segs * tile, heads * hd), jnp.bfloat16),
        grid_spec=pltpu.PrefetchScalarGridSpec(
            num_scalar_prefetch=1,
            grid=(kv, segs),
            in_specs=[
                pl.BlockSpec((tile, group * hd), lambda k, d, s: (d, k)),
                pl.BlockSpec((tile, hd), lambda k, d, s: (d * step + base, 0)),
                pl.BlockSpec((tile, hd), lambda k, d, s: (d * step + base, 0)),
                pl.BlockSpec((1, keys, hd), lambda k, d, s: (k, 0, 0)),
                pl.BlockSpec((1, keys, hd), lambda k, d, s: (k, 0, 0)),
            ],
            out_specs=pl.BlockSpec((tile, group * hd), lambda k, d, s: (d, k)),
            scratch_shapes=[
                pltpu.VMEM((rows, hd), jnp.bfloat16),
                pltpu.VMEM((rows, hd), jnp.float32),
                pltpu.VMEM((rows, hd), jnp.float32),
                pltpu.VMEM((rows, hd), jnp.float32),
            ],
        ),
        compiler_params=pltpu.CompilerParams(dimension_semantics=("arbitrary", "arbitrary")),
        cost_estimate=pl.CostEstimate(flops=4 * segs * tile * heads * (window + tile) * hd, bytes_accessed=4 * keys * kv * hd + 6 * segs * tile * heads * hd, transcendentals=segs * tile * heads * (window + tile)),
        name="window_attention",
    )(start, q_lin, cos, sin, k_all, v_all)


def kv_kernel(*refs, parts, segs, tile, kv, hd, window):
    lin_refs = refs[:parts]
    cos_ref, sin_ref, k_old_ref, v_old_ref, k_ref, v_ref = refs[parts:]
    k_ref[:, :window, :] = k_old_ref[...]
    v_ref[:, :window, :] = v_old_ref[...]
    even = lax.rem(lax.broadcasted_iota(jnp.int32, (tile, hd), 1), 2) == 0
    for c in range(parts):
        for d in range(segs):
            first = (d * parts + c) * tile
            cos = cos_ref[first:first + tile, :]
            sin = sin_ref[first:first + tile, :]
            for h in range(kv):
                kh = lin_refs[c][d * tile:(d + 1) * tile, h * hd:(h + 1) * hd]
                vh = lin_refs[c][d * tile:(d + 1) * tile, (kv + h) * hd:(kv + h + 1) * hd]
                sw = jnp.where(even, pltpu.roll(kh, hd - 1, 1), pltpu.roll(kh, 1, 1))
                k_ref[h, window + first:window + first + tile, :] = (kh * cos + sw * sin).astype(jnp.bfloat16)
                v_ref[h, window + first:window + first + tile, :] = vh.astype(jnp.bfloat16)


def gather_keys(lins, cos, sin, k_old, v_old, *, segs, tile, kv, hd, q_cols):
    parts = len(lins)
    window = k_old.shape[1]
    chunk_len = parts * segs * tile
    width = 2 * kv * hd
    whole = lambda shape: pl.BlockSpec(shape, lambda i: (0,) * len(shape))
    out = jax.ShapeDtypeStruct((kv, window + chunk_len, hd), jnp.bfloat16)
    return pl.pallas_call(
        functools.partial(kv_kernel, parts=parts, segs=segs, tile=tile, kv=kv, hd=hd, window=window),
        out_shape=(out, out),
        grid=(1,),
        in_specs=[pl.BlockSpec((segs * tile, width), lambda i: (0, q_cols // width))] * parts
        + [whole(cos.shape), whole(sin.shape), whole(k_old.shape), whole(v_old.shape)],
        out_specs=(whole(out.shape), whole(out.shape)),
        cost_estimate=pl.CostEstimate(flops=8 * chunk_len * width, bytes_accessed=4 * out.size * 2, transcendentals=0),
        name="window_keys",
    )(*lins, cos, sin, k_old, v_old)


def swiglu_kernel(m_ref, g_ref, u_ref, o_ref):
    m = m_ref[...]
    gate = jnp.dot(m, g_ref[...], preferred_element_type=jnp.float32)
    up = jnp.dot(m, u_ref[...], preferred_element_type=jnp.float32)
    o_ref[...] = (gate * jax.nn.sigmoid(gate) * up).astype(jnp.bfloat16)


def swiglu(m, w_gate, w_up, cols=256):
    rows, depth = m.shape
    ffn = w_gate.shape[1]
    return pl.pallas_call(
        swiglu_kernel,
        out_shape=jax.ShapeDtypeStruct((rows, ffn), jnp.bfloat16),
        grid=(ffn // cols,),
        in_specs=[
            pl.BlockSpec((rows, depth), lambda j: (0, 0)),
            pl.BlockSpec((depth, cols), lambda j: (0, j)),
            pl.BlockSpec((depth, cols), lambda j: (0, j)),
        ],
        out_specs=pl.BlockSpec((rows, cols), lambda j: (0, j)),
        compiler_params=pltpu.CompilerParams(dimension_semantics=("arbitrary",), vmem_limit_bytes=56 * 1024 * 1024),
        cost_estimate=pl.CostEstimate(flops=4 * rows * depth * ffn, bytes_accessed=4 * depth * ffn + 2 * rows * (depth + ffn), transcendentals=rows * ffn),
        name="gate_up",
    )(m, w_gate, w_up)


def rms_norm(rows, gain):
    rows32 = rows.astype(jnp.float32)
    inv_rms = lax.rsqrt(jnp.mean(rows32 * rows32, axis=-1, keepdims=True) + NORM_EPS)
    return (rows32 * inv_rms * gain.astype(jnp.float32)).astype(jnp.bfloat16)


def rope_tables(start, chunk_len, head_dim):
    lane = jnp.arange(head_dim)
    inv_freq = jnp.power(ROPE_BASE, -(lane - lane % 2).astype(jnp.float32) / head_dim)
    angles = (start + jnp.arange(chunk_len)).astype(jnp.float32)[:, None] * inv_freq[None, :]
    return jnp.cos(angles), jnp.sin(angles) * jnp.where(lane % 2 == 0, -1.0, 1.0)


def roll_rows(rows, shift):
    doubled = jnp.concatenate([rows, rows], axis=1)
    return lax.dynamic_slice_in_dim(doubled, shift, rows.shape[1], axis=1)


def write_chunk(cache, chunk, start):
    window = cache.shape[0]
    kv, chunk_len, hd = chunk.shape
    new_rows = chunk.transpose(1, 0, 2)
    filler = jnp.zeros((window - chunk_len, kv, hd), new_rows.dtype)
    doubled = jnp.concatenate([new_rows, filler, new_rows, filler], axis=0)
    placed = lax.dynamic_slice_in_dim(doubled, window - jnp.mod(start, window), window, axis=0)
    offsets = jnp.mod(jnp.arange(window) - start, window)
    return jnp.where((offsets < chunk_len)[:, None, None], placed, cache)


def solution(mesh):
    row_spec = P('dp', 'tp', None)
    cache_spec = P('dp', None, 'tp', None)
    head_cols = P(None, 'tp', None)
    in_specs = (row_spec, P('dp'), cache_spec, cache_spec, P(), head_cols, head_cols, head_cols, P('tp', None, None), P(), P(None, 'tp'), P(None, 'tp'), P('tp', None))
    out_specs = (row_spec, cache_spec, cache_spec)
    segs = mesh.shape['tp']
    parts = 4

    def local_layer(x_in, start_pos, k_cache, v_cache, attn_gain, w_query, w_key, w_value, w_out, mlp_gain, w_gate, w_up, w_down):
        _, seg_len, model_dim = x_in.shape
        _, heads, hd = w_query.shape
        kv = w_key.shape[1]
        window = k_cache.shape[1]
        tile = seg_len // parts
        chunk_len = seg_len * segs
        start = start_pos[0]
        x_parts = [x_in[0, c * tile:(c + 1) * tile] for c in range(parts)]

        def gather(part):
            return lax.all_gather(part, 'tp', axis=0, tiled=True)

        def scatter(part):
            return lax.psum_scatter(part, 'tp', scatter_dimension=0, tiled=True)

        w_qkv = jnp.concatenate([w.reshape(model_dim, -1) for w in (w_query, w_key, w_value)], axis=1)
        cos, sin = rope_tables(start, chunk_len, hd)
        shift = jnp.mod(start, window)
        k_old = roll_rows(k_cache[0].transpose(1, 0, 2), shift)
        v_old = roll_rows(v_cache[0].transpose(1, 0, 2), shift)
        lins = [jnp.dot(gather(rms_norm(x_parts[c], attn_gain)), w_qkv, preferred_element_type=jnp.float32) for c in range(parts)]
        k_all, v_all = gather_keys(lins, cos, sin, k_old, v_old, segs=segs, tile=tile, kv=kv, hd=hd, q_cols=heads * hd)

        w_out2 = w_out.reshape(heads * hd, model_dim)
        plan = (1408, 1408, 1, 1408)
        tie = lax.optimization_barrier
        sums, hiddens, normed, gathered = [None] * parts, [None] * parts, [None] * parts, [None] * parts

        def settle(c):
            hiddens[c] = (x_parts[c].astype(jnp.float32) + sums[c].astype(jnp.float32)).astype(jnp.bfloat16)
            normed[c] = rms_norm(hiddens[c], mlp_gain)
            gathered[c] = gather(normed[c])

        for c in range(parts):
            lin = lins[c]
            if c >= 2:
                lin, normed[c - 2] = tie((lin, normed[c - 2]))
            mixed = attention(lin, cos, sin, k_all, v_all, start_pos, segs=segs, seg_len=seg_len, first=c * tile, tile=tile, heads=heads, window=window, plan=plan, halves=1)
            if c >= 1:
                mixed, sums[c - 1] = tie((mixed, sums[c - 1]))
                settle(c - 1)
            sums[c] = scatter(jnp.dot(mixed, w_out2, preferred_element_type=jnp.float32).astype(jnp.bfloat16))

        x_out = jnp.zeros((seg_len, model_dim), jnp.bfloat16)
        mlp_sums = [None] * parts

        def finish(x_out, c):
            rows = (hiddens[c].astype(jnp.float32) + mlp_sums[c].astype(jnp.float32)).astype(jnp.bfloat16)
            return lax.dynamic_update_slice_in_dim(x_out, rows, c * tile, axis=0)

        for c in range(parts):
            mlp_rows = gathered[c]
            if c == 0:
                mlp_rows, normed[parts - 2] = tie((mlp_rows, normed[parts - 2]))
            if c == 1:
                mlp_rows, normed[parts - 1] = tie((mlp_rows, normed[parts - 1]))
            activated = swiglu(mlp_rows, w_gate, w_up)
            if c == 0:
                activated, sums[parts - 1] = tie((activated, sums[parts - 1]))
                settle(parts - 1)
            else:
                activated, mlp_sums[c - 1] = tie((activated, mlp_sums[c - 1]))
                x_out = finish(x_out, c - 1)
            part = jnp.dot(activated, w_down, preferred_element_type=jnp.float32).astype(jnp.bfloat16)
            part, x_out = tie((part, x_out))
            mlp_sums[c] = scatter(part)
        k_tail, v_tail, part = tie((k_all[:, window:], v_all[:, window:], part))
        x_out = finish(x_out, parts - 1)[None]
        k_new = write_chunk(k_cache[0], k_tail, start)[None]
        v_new = write_chunk(v_cache[0], v_tail, start)[None]
        return x_out, k_new, v_new

    return jax.shard_map(local_layer, mesh=mesh, in_specs=in_specs, out_specs=out_specs, check_vma=False)
```

```python
import functools

import jax
import jax.numpy as jnp
from jax import lax
from jax.experimental import pallas as pl
from jax.experimental.pallas import tpu as pltpu
from jax.sharding import PartitionSpec as P

ROPE_BASE = 10000.0
NORM_EPS = 1e-5
NEG = -1e30


def attn_kernel(info_ref, q_ref, k_ref, vt_ref, o_ref, qt_s, m_s, l_s, acc_s, *,
                tile, group, window, widths, unit, depth, cexp):
    r = pl.program_id(1)
    i0 = pl.multiple_of(info_ref[1 + r], tile)
    hd = k_ref.shape[-1]
    cols = tile * group
    for g in range(group):
        qt_s[:, g * tile:(g + 1) * tile] = q_ref[:, g * hd:(g + 1) * hd].T
    m_s[...] = jnp.full_like(m_s, NEG)
    l_s[...] = jnp.zeros_like(l_s)
    acc_s[...] = jnp.zeros_like(acc_s)
    key = lax.broadcasted_iota(jnp.int32, (tile, unit), 0)
    tok = lax.rem(lax.broadcasted_iota(jnp.int32, (tile, unit), 1), tile)

    def sweep(floor):
        units = []
        offs = [sum(widths[:b]) for b in range(len(widths))]
        for b in reversed(range(len(widths))):
            for u in range(cols // unit):
                units.append((b, u))

        def scores(b, u):
            kb = k_ref[0, pl.ds(i0 + offs[b], widths[b]), :]
            return jnp.dot(kb, qt_s[:, u * unit:(u + 1) * unit], preferred_element_type=jnp.float32)

        def consume(b, u, s):
            w, off = widths[b], offs[b]
            if b == 0:
                piece = jnp.where(key > tok, s[:tile], NEG)
                s = jnp.concatenate([piece, s[tile:]], axis=0)
            if b == len(widths) - 1:
                piece = jnp.where(key <= tok, s[w - tile:], NEG)
                s = jnp.concatenate([s[:w - tile], piece], axis=0)
            if floor is not None:
                vid = i0 + off + lax.broadcasted_iota(jnp.int32, (w, 1), 0)
                s = jnp.where(vid >= floor, s, NEG)
            sl = slice(u * unit, (u + 1) * unit)
            m_prev = m_s[:, sl]
            m_new = jnp.maximum(m_prev, jnp.max(s, axis=0, keepdims=True))
            m_s[:, sl] = m_new
            alpha = jnp.exp2((m_prev - m_new) * cexp)
            p = jnp.exp2((s - m_new) * cexp)
            l_s[:, sl] = l_s[:, sl] * alpha + jnp.sum(p, axis=0, keepdims=True)
            vb = vt_ref[0, :, pl.ds(i0 + off, w)]
            acc_s[:, sl] = acc_s[:, sl] * alpha + jnp.dot(vb, p.astype(jnp.bfloat16), preferred_element_type=jnp.float32)

        ahead = [scores(*x) for x in units[:depth]]
        for n, x in enumerate(units):
            if n + depth < len(units):
                ahead.append(scores(*units[n + depth]))
            consume(*x, ahead.pop(0))

    lowest = window - info_ref[0]

    @pl.when(lowest <= i0)
    def _():
        sweep(None)

    @pl.when(lowest > i0)
    def _():
        sweep(lowest)

    for g in range(group):
        sl = slice(g * tile, (g + 1) * tile)
        o_ref[:, g * hd:(g + 1) * hd] = (acc_s[:, sl] / l_s[:, sl]).T.astype(jnp.bfloat16)


def attention(q, k_all, vt_all, info, *, segs, tile, heads, window, per_seg=1, place=0, widths=(1408, 1408, 1408), unit=256, depth=1, flags=None):
    kv, keys, hd = k_all.shape
    group = heads // kv
    assert sum(widths) == window + tile
    kern = functools.partial(attn_kernel, tile=tile, group=group, window=window, widths=widths, unit=unit, depth=depth,
                             cexp=float(hd ** -0.5 * 1.4426950408889634))
    cols = tile * group
    return pl.pallas_call(
        kern,
        out_shape=jax.ShapeDtypeStruct((segs * tile, heads * hd), jnp.bfloat16),
        grid_spec=pltpu.PrefetchScalarGridSpec(
            num_scalar_prefetch=1,
            grid=(kv, segs),
            in_specs=[
                pl.BlockSpec((tile, group * hd), lambda k, d, s: (d * per_seg + place, k)),
                pl.BlockSpec((1, keys, hd), lambda k, d, s: (k, 0, 0)),
                pl.BlockSpec((1, hd, keys), lambda k, d, s: (k, 0, 0)),
            ],
            out_specs=pl.BlockSpec((tile, group * hd), lambda k, d, s: (d, k)),
            scratch_shapes=[
                pltpu.VMEM((hd, cols), jnp.bfloat16),
                pltpu.VMEM((1, cols), jnp.float32),
                pltpu.VMEM((1, cols), jnp.float32),
                pltpu.VMEM((hd, cols), jnp.float32),
            ],
        ),
        compiler_params=pltpu.CompilerParams(dimension_semantics=("arbitrary", "arbitrary"), flags=flags or {}),
        cost_estimate=pl.CostEstimate(flops=4 * segs * tile * heads * (window + tile) * hd, bytes_accessed=4 * keys * kv * hd + 4 * segs * tile * heads * hd, transcendentals=segs * tile * heads * (window + tile)),
        name="window_attention",
    )(info, q, k_all, vt_all)


def qkv_kernel(n_ref, wq_ref, wk_ref, wv_ref, cos_ref, sin_ref, q_ref, k_ref, v_ref, *, q_steps):
    step = pl.program_id(0)
    rows, hd = n_ref.shape[0], cos_ref.shape[-1]

    def times(w_ref):
        heads = [w_ref[h] for h in range(w_ref.shape[0])]
        return jnp.dot(n_ref[...], jnp.concatenate(heads, axis=1), preferred_element_type=jnp.float32)

    def turned(lin, out_ref):
        cos = cos_ref[...].reshape(rows, hd)
        sin = sin_ref[...].reshape(rows, hd)
        even = lax.rem(lax.broadcasted_iota(jnp.int32, (rows, hd), 1), 2) == 0
        for h in range(lin.shape[1] // hd):
            lh = lin[:, h * hd:(h + 1) * hd]
            sw = jnp.where(even, pltpu.roll(lh, hd - 1, 1), pltpu.roll(lh, 1, 1))
            out_ref[:, h * hd:(h + 1) * hd] = (lh * cos + sw * sin).astype(jnp.bfloat16)

    @pl.when(step < q_steps)
    def _():
        turned(times(wq_ref), q_ref)

    @pl.when(step == q_steps)
    def _():
        turned(times(wk_ref), k_ref)

    @pl.when(step == q_steps + 1)
    def _():
        v_ref[...] = times(wv_ref).astype(jnp.bfloat16)


def project(normed, w_q, w_k, w_v, cos, sin, part, segs, step_heads=2):
    rows, depth = normed.shape
    hd = cos.shape[-1]
    heads, kv = w_q.shape[0], w_k.shape[0]
    q_steps = heads // step_heads
    fixed = lambda shape: pl.BlockSpec(shape, lambda j: (0,) * len(shape))
    table = pl.BlockSpec((segs, rows // segs, hd), lambda j: (0, part, 0))
    return pl.pallas_call(
        functools.partial(qkv_kernel, q_steps=q_steps),
        out_shape=tuple(jax.ShapeDtypeStruct((rows, h * hd), jnp.bfloat16) for h in (heads, kv, kv)),
        grid=(q_steps + 2,),
        in_specs=[fixed((rows, depth)), pl.BlockSpec((step_heads, depth, hd), lambda j: (jnp.minimum(j, q_steps - 1), 0, 0)), fixed(w_k.shape), fixed(w_v.shape), table, table],
        out_specs=(pl.BlockSpec((rows, step_heads * hd), lambda j: (0, jnp.minimum(j, q_steps - 1))), fixed((rows, kv * hd)), fixed((rows, kv * hd))),
        compiler_params=pltpu.CompilerParams(dimension_semantics=("arbitrary",), vmem_limit_bytes=56 * 1024 * 1024),
        cost_estimate=pl.CostEstimate(flops=2 * rows * depth * hd * (heads + 2 * kv), bytes_accessed=2 * depth * hd * (heads + 2 * kv) + 2 * rows * depth, transcendentals=0),
        name="project_qkv",
    )(normed, w_q, w_k, w_v, cos, sin)


def keys_kernel(*refs, groups, segs, seg_len, kv, hd, window):
    count = len(groups)
    k_parts, v_parts = refs[:count], refs[count:2 * count]
    k_old_ref, vt_old_ref, k_ref, vt_ref = refs[2 * count:]
    k_ref[:, :window, :] = k_old_ref[...]
    vt_ref[:, :, :window] = vt_old_ref[...]
    for n, (base, size) in enumerate(groups):
        for d in range(segs):
            first = window + d * seg_len + base
            for h in range(kv):
                k_ref[h, first:first + size, :] = k_parts[n][d * size:(d + 1) * size, h * hd:(h + 1) * hd]
                vt_ref[h, :, first:first + size] = v_parts[n][d * size:(d + 1) * size, h * hd:(h + 1) * hd].T


def gather_keys(ks, vs, k_old, vt_old, groups, segs, seg_len):
    kv, window, hd = k_old.shape
    keys = window + segs * seg_len
    return pl.pallas_call(
        functools.partial(keys_kernel, groups=groups, segs=segs, seg_len=seg_len, kv=kv, hd=hd, window=window),
        out_shape=(jax.ShapeDtypeStruct((kv, keys, hd), jnp.bfloat16), jax.ShapeDtypeStruct((kv, hd, keys), jnp.bfloat16)),
        cost_estimate=pl.CostEstimate(flops=kv * keys * hd, bytes_accessed=8 * kv * keys * hd, transcendentals=0),
        name="window_keys",
    )(*ks, *vs, k_old, vt_old)


def swiglu_kernel(m_ref, g_ref, u_ref, o_ref):
    m = m_ref[...]
    gate = jnp.dot(m, g_ref[...], preferred_element_type=jnp.float32)
    up = jnp.dot(m, u_ref[...], preferred_element_type=jnp.float32)
    o_ref[...] = (gate * jax.nn.sigmoid(gate) * up).astype(jnp.bfloat16)


def swiglu(m, w_gate, w_up, cols=256):
    rows, depth = m.shape
    ffn = w_gate.shape[1]
    return pl.pallas_call(
        swiglu_kernel,
        out_shape=jax.ShapeDtypeStruct((rows, ffn), jnp.bfloat16),
        grid=(ffn // cols,),
        in_specs=[
            pl.BlockSpec((rows, depth), lambda j: (0, 0)),
            pl.BlockSpec((depth, cols), lambda j: (0, j)),
            pl.BlockSpec((depth, cols), lambda j: (0, j)),
        ],
        out_specs=pl.BlockSpec((rows, cols), lambda j: (0, j)),
        compiler_params=pltpu.CompilerParams(dimension_semantics=("arbitrary",), vmem_limit_bytes=56 * 1024 * 1024),
        cost_estimate=pl.CostEstimate(flops=4 * rows * depth * ffn, bytes_accessed=4 * depth * ffn + 2 * rows * (depth + ffn), transcendentals=rows * ffn),
        name="gate_up",
    )(m, w_gate, w_up)


def product_kernel(a_ref, b_ref, o_ref):
    o_ref[...] = jnp.dot(a_ref[...], b_ref[...], preferred_element_type=jnp.float32).astype(jnp.bfloat16)


def product(a, b, cols, name):
    rows, depth = a.shape
    width = b.shape[1]
    return pl.pallas_call(
        product_kernel,
        out_shape=jax.ShapeDtypeStruct((rows, width), jnp.bfloat16),
        grid=(width // cols,),
        in_specs=[pl.BlockSpec((rows, depth), lambda j: (0, 0)), pl.BlockSpec((depth, cols), lambda j: (0, j))],
        out_specs=pl.BlockSpec((rows, cols), lambda j: (0, j)),
        compiler_params=pltpu.CompilerParams(dimension_semantics=("arbitrary",), vmem_limit_bytes=56 * 1024 * 1024),
        cost_estimate=pl.CostEstimate(flops=2 * rows * depth * width, bytes_accessed=2 * (depth * width + rows * (depth + width)), transcendentals=0),
        name=name,
    )(a, b)


def rms_norm(rows, gain):
    rows32 = rows.astype(jnp.float32)
    inv_rms = lax.rsqrt(jnp.mean(rows32 * rows32, axis=-1, keepdims=True) + NORM_EPS)
    return (rows32 * inv_rms * gain.astype(jnp.float32)).astype(jnp.bfloat16)


def rope_tables(start, chunk_len, head_dim):
    lane = jnp.arange(head_dim)
    inv_freq = jnp.power(ROPE_BASE, -(lane - lane % 2).astype(jnp.float32) / head_dim)
    angles = (start + jnp.arange(chunk_len)).astype(jnp.float32)[:, None] * inv_freq[None, :]
    return jnp.cos(angles), jnp.sin(angles) * jnp.where(lane % 2 == 0, -1.0, 1.0)


def roll_rows(rows, shift):
    doubled = jnp.concatenate([rows, rows], axis=1)
    return lax.dynamic_slice_in_dim(doubled, shift, rows.shape[1], axis=1)


def write_chunk(cache, new_rows, start):
    window, kv, hd = cache.shape
    chunk_len = new_rows.shape[0]
    filler = jnp.zeros((window - chunk_len, kv, hd), new_rows.dtype)
    doubled = jnp.concatenate([new_rows, filler, new_rows, filler], axis=0)
    placed = lax.dynamic_slice_in_dim(doubled, window - jnp.mod(start, window), window, axis=0)
    offsets = jnp.mod(jnp.arange(window) - start, window)
    return jnp.where((offsets < chunk_len)[:, None, None], placed, cache)


def solution(mesh):
    row_spec = P('dp', 'tp', None)
    cache_spec = P('dp', None, 'tp', None)
    head_cols = P(None, 'tp', None)
    in_specs = (row_spec, P('dp'), cache_spec, cache_spec, P(), head_cols, head_cols, head_cols, P('tp', None, None), P(), P(None, 'tp'), P(None, 'tp'), P('tp', None))
    out_specs = (row_spec, cache_spec, cache_spec)
    segs = mesh.shape['tp']
    parts = 4

    def local_layer(x_in, start_pos, k_cache, v_cache, attn_gain, w_query, w_key, w_value, w_out, mlp_gain, w_gate, w_up, w_down):
        _, seg_len, model_dim = x_in.shape
        _, heads, hd = w_query.shape
        kv = w_key.shape[1]
        window = k_cache.shape[1]
        tile = seg_len // parts
        chunk_len = seg_len * segs
        start = start_pos[0]
        x_parts = [x_in[0, c * tile:(c + 1) * tile] for c in range(parts)]
        tie = lax.optimization_barrier

        def gather(part):
            return lax.all_gather(part, 'tp', axis=0, tiled=True)

        def scatter(part):
            return lax.psum_scatter(part, 'tp', scatter_dimension=0, tiled=True)

        w_q, w_k, w_v = [w.transpose(1, 0, 2) for w in (w_query, w_key, w_value)]
        cos, sin = [t.reshape(segs, seg_len, hd) for t in rope_tables(start, chunk_len, hd)]
        shift = jnp.mod(start, window)
        k_old = roll_rows(k_cache[0].transpose(1, 0, 2), shift)
        vt_old = roll_rows(v_cache[0].transpose(1, 0, 2), shift).transpose(0, 2, 1)
        groups = ((0, 2 * tile), (2 * tile, tile), (3 * tile, tile))
        ks, vs, q_of = [], [], []
        ahead = None
        for base, size in groups:
            x_rows = x_in[0, base:base + size]
            if ahead is not None:
                x_rows, ahead = tie((x_rows, ahead))
            ahead = rms_norm(x_rows, attn_gain)
            rows = gather(ahead)
            if ks:
                rows, ks[-1] = tie((rows, ks[-1]))
            q, k, v = project(rows, w_q, w_k, w_v, cos, sin, base // size, segs)
            ks.append(k)
            vs.append(v)
            q_of += [(q, size // tile, t) for t in range(size // tile)]
        k_all, vt_all = gather_keys(ks, vs, k_old, vt_old, groups, segs, seg_len)

        w_out2 = w_out.reshape(heads * hd, model_dim)
        sums, hiddens, normed, gathered = [None] * parts, [None] * parts, [None] * parts, [None] * parts

        def settle(c):
            hiddens[c] = (x_parts[c].astype(jnp.float32) + sums[c].astype(jnp.float32)).astype(jnp.bfloat16)
            normed[c] = rms_norm(hiddens[c], mlp_gain)
            gathered[c] = gather(normed[c])

        def token_rows(chunks):
            rows = [chunk.reshape(segs, -1, kv, hd) for chunk in chunks]
            return jnp.concatenate(rows, axis=1).reshape(chunk_len, kv, hd)

        for c in range(parts):
            q, per_seg, place = q_of[c]
            if c == 3:
                q, normed[0], k_new, v_new = tie((q, normed[0], k_new, v_new))
            info = jnp.concatenate([start_pos, c * tile + seg_len * jnp.arange(segs, dtype=jnp.int32)])
            mixed = attention(q, k_all, vt_all, info, segs=segs, tile=tile, heads=heads, window=window, per_seg=per_seg, place=place,
                              unit=256, depth=2)
            if c == 1:
                ks, vs, mixed = tie((ks, vs, mixed))
                k_new = write_chunk(k_cache[0], token_rows(ks), start)
                v_new = write_chunk(v_cache[0], token_rows(vs), start)
            if c >= 2:
                mixed, sums[c - 2] = tie((mixed, sums[c - 2]))
                settle(c - 2)
            sums[c] = scatter(product(mixed, w_out2, 1024, "heads_out"))

        x_out = jnp.zeros((seg_len, model_dim), jnp.bfloat16)
        mlp_sums = [None] * parts

        def finish(x_out, c):
            rows = (hiddens[c].astype(jnp.float32) + mlp_sums[c].astype(jnp.float32)).astype(jnp.bfloat16)
            return lax.dynamic_update_slice_in_dim(x_out, rows, c * tile, axis=0)

        for c in range(parts):
            mlp_rows = gathered[c]
            if c < 3:
                mlp_rows, normed[1 + c] = tie((mlp_rows, normed[1 + c]))
            if c > 0:
                mlp_rows, part = tie((mlp_rows, part))
                mlp_sums[c - 1] = scatter(part)
            activated = swiglu(mlp_rows, w_gate, w_up)
            if c < 2:
                activated, sums[2 + c] = tie((activated, sums[2 + c]))
                settle(2 + c)
            if c == 3:
                activated, mlp_sums[0], mlp_sums[1] = tie((activated, mlp_sums[0], mlp_sums[1]))
                x_out = finish(finish(x_out, 0), 1)
            part = product(activated, w_down, 512, "mlp_down")
            if c == 3:
                part, x_out = tie((part, x_out))
                mlp_sums[c] = scatter(part)
        x_out = finish(finish(x_out, 2), 3)
        return x_out[None], k_new[None], v_new[None]

    return jax.shard_map(local_layer, mesh=mesh, in_specs=in_specs, out_specs=out_specs, check_vma=False)
```
